256 devices in a mesh: row: 32 (over y_hi, z, core), col: 8 (over x, y_lo).
Axes of the slice: x: 4, y: 4 (y_hi: 2, y_lo: 2; y = y_hi * 2 + y_lo), z: 8, core: 2. Of those that a mesh axis runs over, the one named last changes fastest.
Arguments:
- hidden: bfloat16 [32768, 768], P(('row', 'col')), may hold values from -6 to 6
- projection: bfloat16 [768, 512], replicated, may hold values from -0.21875 to 0.21875
- alpha: bfloat16 [32768], P(('row', 'col')), may hold values from -6 to 6
- probe_pairs: bfloat16 [32768, 32], P(('row', 'col')), may hold values from -6 to 6
- amplitude: float32 [1], replicated, may hold values from 0.5 to 2
- length_sq: float32 [1], replicated, may hold values from 512 to 1024
Outputs:
- grad_hidden: bfloat16 [32768, 768], P(('row', 'col'))
- grad_proj: float32 [768, 512], P('row')
The draws below stay inside these ranges and needn't reach their ends.
All inputs are finite; a program needn't handle non-finite values.
Results may differ from the reference program's by a relative error of at most 0.023.
Values may be sent and summed in bfloat16 or wider, within the bound.
No kernel may reach another device: no remote copies, remote signals or barrier semaphores. Data moves between devices by JAX's collectives and lax.ppermute only.
A program may use at most 64 MiB of HBM per device.

```python
import math
import jax
import jax.numpy as jnp
from jax import lax

HID = 768
FEAT = 512
PROBES = 16
POINTS = 32768
N_ROW = 32


def draw_hidden(key, part):
    groups = max(POINTS // 256, 2)
    centers = jax.random.normal(jax.random.fold_in(key, 13), (groups, HID), jnp.float32)
    labels = jax.random.randint(jax.random.fold_in(key, 14), (POINTS,), 0, groups)
    placed = 2.0 * jnp.take(centers, labels, axis=0)
    values = placed + jax.random.normal(jax.random.fold_in(key, 11), (POINTS, HID), jnp.float32)
    values = jnp.clip(values, -6.0, 6.0)
    return values.astype(jnp.bfloat16)


def level_of(key, extent, pieces, smallest, top_value):
    loudness, own = 1.0, jax.random.fold_in(key, 6)
    for dim, blocks in pieces:
        heights = jnp.exp(jax.random.uniform(jax.random.fold_in(own, dim), (blocks,), jnp.float32, smallest / len(pieces), top_value / len(pieces)))
        loudness = loudness * jnp.repeat(heights, extent[dim] // blocks).reshape([-1 if axis == dim else 1 for axis in range(len(extent))])
    return loudness


def bell_draw(own_key, extent, width, bound, pieces=(), held_as=jnp.bfloat16):
    entries = width * jax.random.normal(own_key, extent, jnp.float32)
    if pieces:
        entries = entries * level_of(own_key, extent, pieces, -0.22, 0.18)
    return jnp.clip(entries, -bound, bound).astype(held_as)


def setup_inputs(seed: int = 0) -> dict:
    key_of = jax.random.split(jax.random.key(seed), 7)
    return {
        "hidden": draw_hidden(jax.random.fold_in(key_of[6], 71), 0),
        "projection": bell_draw(key_of[1], (HID, FEAT), HID ** -0.5, 0.21875),
        "alpha": bell_draw(key_of[2], (POINTS,), 1.0, 6.0, ((0, 256),)),
        "probe_pairs": bell_draw(key_of[3], (POINTS, 2 * PROBES), 1.0, 6.0, ((0, 256),)),
        "amplitude": jnp.clip(jnp.exp(jax.random.uniform(key_of[4], (1,), jnp.float32, math.log(0.5), math.log(2.0))), 0.5, 2.0),
        "length_sq": jnp.clip(jnp.exp(jax.random.uniform(key_of[5], (1,), jnp.float32, math.log(512.0), math.log(1024.0))), 512.0, 1024.0),
    }


def right_of(factors, probes):
    scale = 1.0 / (4 * probes)
    return jnp.concatenate([factors[:, :1] * 0.5, factors[:, 1 + probes:] * (-scale), factors[:, 1:1 + probes] * (-scale)], axis=1)


def reference(hidden, projection, alpha, probe_pairs, amplitude, length_sq):
    feats = jnp.dot(hidden, projection, preferred_element_type=jnp.float32).astype(jnp.bfloat16)
    left = jnp.concatenate([alpha[:, None], probe_pairs], axis=1)
    probes = probe_pairs.shape[1] // 2
    right = right_of(left, probes)
    amp = amplitude[0]
    lsq = length_sq[0]
    feat_f = feats.astype(jnp.float32)
    sq_all = jnp.sum(feat_f * feat_f, axis=1)
    block = POINTS // N_ROW

    def one_block(index):
        start = (index * block).astype(jnp.int32)
        rows_feat = lax.dynamic_slice_in_dim(feats, start, block, 0)
        rows_left = lax.dynamic_slice_in_dim(left, start, block, 0)
        rows_sq = lax.dynamic_slice_in_dim(sq_all, start, block, 0)
        inner = jnp.dot(rows_feat, feats.T, preferred_element_type=jnp.float32)
        dist = rows_sq[:, None] + sq_all[None, :] - 2.0 * inner
        kern = amp * jnp.exp(-0.5 * dist / lsq)
        gmat = jnp.dot(rows_left, right.T, preferred_element_type=jnp.float32)
        weight = gmat * kern
        rowsum = jnp.sum(weight, axis=1)
        moved = jnp.dot(weight.astype(jnp.bfloat16), feats, preferred_element_type=jnp.float32)
        return moved, rowsum

    moved, rowsum = lax.map(one_block, jnp.arange(N_ROW, dtype=jnp.int32))
    moved = moved.reshape(POINTS, -1)
    rowsum = rowsum.reshape(POINTS)
    grad_feat = ((2.0 / lsq) * (moved - rowsum[:, None] * feat_f)).astype(jnp.bfloat16)
    grad_hidden = jnp.dot(grad_feat, projection.T, preferred_element_type=jnp.float32).astype(jnp.bfloat16)
    grad_proj = lax.dot_general(hidden, grad_feat, (((0,), (0,)), ((), ())), preferred_element_type=jnp.float32)
    return grad_hidden, grad_proj
```

```python
import functools

import jax
import jax.numpy as jnp
from jax import lax
from jax.experimental import pallas as pl
from jax.experimental.pallas import tpu as pltpu
from jax.sharding import Mesh, PartitionSpec as P

LOG2E = 1.4426950408889634
PTS = 128
FEAT = 512
MSG = 560
ROW_CHUNK = 256
COL_CHUNK = 1024
ALL = ("yh", "z", "c", "x", "yl")
VMEM = pl.BlockSpec(memory_space=pltpu.VMEM)
SMEM = pl.BlockSpec(memory_space=pltpu.SMEM)


def pair_kernel(n, amp_ref, lsq_ref, rows_ref, *refs):
    cols_refs = refs[:n]
    out_ref, rf, la, ai, cf, cfac, acc, rs = refs[n:]
    nb = rows_ref.shape[0]
    rows = nb * PTS
    chunk = COL_CHUNK
    c1 = LOG2E / lsq_ref[0]
    half = 0.5 * c1
    lane = lax.broadcasted_iota(jnp.int32, (PTS, 128), 1)
    for b in range(nb):
        here = slice(b * PTS, (b + 1) * PTS)
        for k in range(4):
            rf[here, k * 128 : (k + 1) * 128] = rows_ref[b, k * 128 : (k + 1) * 128, :]
        fac = rows_ref[b, FEAT:MSG, :].astype(jnp.float32)
        sq = fac[33:34] + fac[34:35] + fac[35:36]
        swapped = jnp.concatenate(
            [
                fac[0:1] * 0.5,
                fac[17:33] * (-1 / 64),
                fac[1:17] * (-1 / 64),
                sq * half,
                jnp.zeros((94, 128), jnp.float32),
            ],
            axis=0,
        ).T
        ai[here, :] = jnp.broadcast_to(swapped[:, 33:34], (PTS, 128))
        la[here, :] = jnp.where(lane < 33, swapped, 0.0).astype(jnp.bfloat16)
    at = 0
    for ref in cols_refs:
        for b in range(ref.shape[0] // MSG):
            for k in range(4):
                cf[at : at + PTS, k * 128 : (k + 1) * 128] = ref[
                    b * MSG + k * 128 : b * MSG + (k + 1) * 128, :
                ]
            j, o = divmod(at, chunk)
            cfac[j, 0:48, o : o + PTS] = ref[b * MSG + FEAT : (b + 1) * MSG, :]
            at += PTS
    acc[...] = jnp.zeros_like(acc)
    rs[...] = jnp.zeros_like(rs)
    cfac[:, 48:, :] = jnp.zeros((at // chunk, 80, chunk), jnp.bfloat16)
    log_amp = jnp.log2(jnp.full((1, chunk), amp_ref[0], jnp.float32))

    def step(j, carry):
        colf = cf[pl.ds(pl.multiple_of(j * chunk, chunk), chunk), :]
        fac = cfac[j]
        f3 = fac[32:40].astype(jnp.float32)
        bj = (f3[1:2] + f3[2:3] + f3[3:4]) * half - log_amp
        for r in range(rows // ROW_CHUNK):
            here = slice(r * ROW_CHUNK, (r + 1) * ROW_CHUNK)
            inner = lax.dot_general(
                rf[here, :], colf, (((1,), (1,)), ((), ())), preferred_element_type=jnp.float32
            )
            gmat = jnp.dot(la[here, :], fac, preferred_element_type=jnp.float32)
            a = jnp.concatenate([ai[here, :]] * (chunk // 128), axis=1)
            w = gmat * jnp.exp2(inner * c1 - a - bj)
            total = w[:, 0:128]
            for q in range(1, chunk // 128):
                total = total + w[:, q * 128 : (q + 1) * 128]
            rs[here, :] += total
            acc[here, :] += jnp.dot(
                w.astype(jnp.bfloat16), colf, preferred_element_type=jnp.float32
            )
        return carry

    lax.fori_loop(0, at // chunk, step, 0)
    scale = 2.0 / lsq_ref[0]
    for r in range(nb):
        here = slice(r * PTS, (r + 1) * PTS)
        rowsum = jnp.sum(rs[here, :], axis=1, keepdims=True)
        out_ref[r] = (scale * (acc[here, :] - rowsum * rf[here, :].astype(jnp.float32))).astype(
            jnp.bfloat16
        )


def pair(rows, cols, amp, lsq):
    nb = rows.shape[0]
    r = nb * PTS
    c = sum(x.shape[0] for x in cols) // MSG * PTS
    return pl.pallas_call(
        functools.partial(pair_kernel, len(cols)),
        out_shape=jax.ShapeDtypeStruct((nb, PTS, FEAT), jnp.bfloat16),
        in_specs=[SMEM, SMEM, VMEM] + [VMEM] * len(cols),
        out_specs=VMEM,
        scratch_shapes=[
            pltpu.VMEM((r, FEAT), jnp.bfloat16),
            pltpu.VMEM((r, 128), jnp.bfloat16),
            pltpu.VMEM((r, 128), jnp.float32),
            pltpu.VMEM((c, FEAT), jnp.bfloat16),
            pltpu.VMEM((c // COL_CHUNK, 128, COL_CHUNK), jnp.bfloat16),
            pltpu.VMEM((r, FEAT), jnp.float32),
            pltpu.VMEM((r, 128), jnp.float32),
        ],
        cost_estimate=pl.CostEstimate(
            flops=2 * r * c * 1280, bytes_accessed=4 * r * FEAT, transcendentals=r * c
        ),
        compiler_params=pltpu.CompilerParams(vmem_limit_bytes=48 * 1024 * 1024),
        name="pair",
    )(amp, lsq, rows, *cols)


def message_kernel(hidden_ref, proj_ref, alpha_ref, probes_ref, out_ref):
    feats = jnp.dot(hidden_ref[...], proj_ref[...], preferred_element_type=jnp.float32).astype(
        jnp.bfloat16
    )
    feat_f = feats.astype(jnp.float32)
    for k in range(4):
        out_ref[k * 128 : (k + 1) * 128, :] = feats[:, k * 128 : (k + 1) * 128]
    sq = jnp.sum(feat_f * feat_f, axis=1, keepdims=True)
    hi = sq.astype(jnp.bfloat16).astype(jnp.float32)
    mid = (sq - hi).astype(jnp.bfloat16).astype(jnp.float32)
    low = sq - hi - mid
    probes = probes_ref[...].astype(jnp.float32)
    wide = jnp.concatenate([probes, hi, mid, low, jnp.zeros((PTS, 93), jnp.float32)], axis=1).T
    fac = jnp.concatenate([alpha_ref[...].astype(jnp.float32), wide[0:47]], axis=0)
    out_ref[FEAT:MSG, :] = fac.astype(jnp.bfloat16)


def message(hidden, projection, alpha, probe_pairs):
    return pl.pallas_call(
        message_kernel,
        out_shape=jax.ShapeDtypeStruct((MSG, 128), jnp.bfloat16),
        in_specs=[VMEM] * 4,
        out_specs=VMEM,
        name="message",
    )(hidden, projection, alpha.reshape(1, PTS), probe_pairs)


def sent_to_all(x, axes, size):
    return lax.all_to_all(jnp.broadcast_to(x[None], (size, *x.shape)), axes, 0, 0, tiled=True)


def shifted(x, axis, by):
    n = lax.axis_size(axis)
    return lax.ppermute(x, axis, [(i, (i + by) % n) for i in range(n)])


def per_device(hidden, projection, alpha, probe_pairs, amplitude, length_sq):
    msg = message(hidden, projection, alpha, probe_pairs)
    rows = sent_to_all(msg, ("x", "yl"), 8)
    both = jnp.concatenate([msg, shifted(msg, "yh", 1)], axis=0)
    held = [both]
    up, down = both, both
    for k in range(4):
        up = shifted(up, "z", 1)
        held.append(up)
        if k < 3:
            down = shifted(down, "z", -1)
            held.append(down)
    cols = held + [shifted(x, "c", 1) for x in held]
    part = pair(rows, cols, amplitude, length_sq)
    arrived = lax.all_to_all(part, ("x", "yl"), 0, 0, tiled=True)
    grad_feat = arrived.astype(jnp.float32).sum(axis=0).astype(jnp.bfloat16)
    grad_hidden = jnp.dot(grad_feat, projection.T, preferred_element_type=jnp.float32).astype(
        jnp.bfloat16
    )
    partial = lax.dot_general(
        hidden, grad_feat, (((0,), (0,)), ((), ())), preferred_element_type=jnp.float32
    ).astype(jnp.bfloat16)
    blocks = partial.reshape(2, 8, 2, 24, FEAT).transpose(2, 1, 0, 3, 4)
    got = lax.all_to_all(blocks, "c", 0, 0, tiled=True)
    core_sum = got.astype(jnp.float32).sum(axis=0).astype(jnp.bfloat16)
    got = lax.all_to_all(core_sum, "z", 0, 0, tiled=True)
    z_sum = got.astype(jnp.float32).sum(axis=0).astype(jnp.bfloat16)
    spread = jnp.broadcast_to(z_sum[:, None], (2, 8, 24, FEAT)).reshape(16, 24, FEAT)
    got = lax.all_to_all(spread, ("yh", "x", "yl"), 0, 0, tiled=True)
    grad_proj = got.astype(jnp.float32).sum(axis=0)
    return grad_hidden, grad_proj


def solution(mesh):
    fine = Mesh(mesh.devices.reshape(2, 8, 2, 4, 2), ALL)
    placed = (P(ALL, None), P(), P(ALL), P(ALL, None), P(), P())
    return jax.shard_map(
        per_device,
        mesh=fine,
        in_specs=placed,
        out_specs=(P(ALL, None), P(("yh", "z", "c"), None)),
        check_vma=False,
    )
```

```python
import functools

import jax
import jax.numpy as jnp
from jax import lax
from jax.experimental import pallas as pl
from jax.experimental.pallas import tpu as pltpu
from jax.sharding import Mesh, PartitionSpec as P


LOG2E = 1.4426950408889634
PTS = 128
FEAT = 512
MSG = 560
ROW_CHUNK = 512
ALL = ("yh", "z", "c", "x", "yl")
VMEM = pl.BlockSpec(memory_space=pltpu.VMEM)
SMEM = pl.BlockSpec(memory_space=pltpu.SMEM)


def prepare_kernel(lsq_ref, near_ref, far_ref, rf, la, ai):
    half = 0.5 * LOG2E / lsq_ref[0]
    lane = lax.broadcasted_iota(jnp.int32, (PTS, 128), 1)
    for side, ref in enumerate((near_ref, far_ref)):
        for b in range(ref.shape[0]):
            at = (side * ref.shape[0] + b) * PTS
            here = slice(at, at + PTS)
            for k in range(4):
                rf[here, k * 128 : (k + 1) * 128] = ref[b, k * 128 : (k + 1) * 128, :]
            fac = ref[b, FEAT:MSG, :].astype(jnp.float32)
            sq = fac[33:34] + fac[34:35] + fac[35:36]
            swapped = jnp.concatenate(
                [
                    fac[0:1] * 0.5,
                    fac[17:33] * (-1 / 64),
                    fac[1:17] * (-1 / 64),
                    sq * half,
                    jnp.zeros((94, 128), jnp.float32),
                ],
                axis=0,
            ).T
            ai[here, :] = jnp.broadcast_to(swapped[:, 33:34], (PTS, 128))
            la[here, :] = jnp.where(lane < 33, swapped, 0.0).astype(jnp.bfloat16)


def prepare(near, far, lsq):
    r = (near.shape[0] + far.shape[0]) * PTS
    return pl.pallas_call(
        prepare_kernel,
        out_shape=(
            jax.ShapeDtypeStruct((r, FEAT), jnp.bfloat16),
            jax.ShapeDtypeStruct((r, 128), jnp.bfloat16),
            jax.ShapeDtypeStruct((r, 128), jnp.float32),
        ),
        in_specs=[SMEM, VMEM, VMEM],
        out_specs=(VMEM, VMEM, VMEM),
        cost_estimate=pl.CostEstimate(flops=r * FEAT * 100, bytes_accessed=r * FEAT, transcendentals=0),
        compiler_params=pltpu.CompilerParams(vmem_limit_bytes=16 * 1024 * 1024),
        name="prepare",
    )(lsq, near, far)


def chunk_kernel(n, first, last, amp_ref, lsq_ref, rf, la, ai, *refs):
    if not first:
        acc_in, rs_in = refs[:2]
        refs = refs[2:]
    cols_refs = refs[:n]
    refs = refs[n:]
    if last:
        out_ref, cf, cfac, acc, rs = refs
    else:
        acc, rs, cf, cfac = refs
    rows, width = rf.shape[0], cf.shape[0]
    c1 = LOG2E / lsq_ref[0]
    half = 0.5 * c1
    at = 0
    for ref in cols_refs:
        for k in range(4):
            cf[at : at + PTS, k * 128 : (k + 1) * 128] = ref[k * 128 : (k + 1) * 128, :]
        cfac[0:48, at : at + PTS] = ref[FEAT:MSG, :]
        at += PTS
    cfac[48:, :] = jnp.zeros((80, width), jnp.bfloat16)
    f3 = cfac[32:40, :].astype(jnp.float32)
    bj = (f3[1:2] + f3[2:3] + f3[3:4]) * half - jnp.log2(
        jnp.full((1, width), amp_ref[0], jnp.float32)
    )
    for r in range(rows // ROW_CHUNK):
        here = slice(r * ROW_CHUNK, (r + 1) * ROW_CHUNK)
        inner = lax.dot_general(
            rf[here, :], cf[...], (((1,), (1,)), ((), ())), preferred_element_type=jnp.float32
        )
        gmat = jnp.dot(la[here, :], cfac[...], preferred_element_type=jnp.float32)
        a = jnp.concatenate([ai[here, :]] * (width // 128), axis=1)
        w = gmat * jnp.exp2(inner * c1 - a - bj)
        total = w[:, 0:128]
        for q in range(1, width // 128):
            total = total + w[:, q * 128 : (q + 1) * 128]
        moved = jnp.dot(w.astype(jnp.bfloat16), cf[...], preferred_element_type=jnp.float32)
        if not first:
            total = rs_in[here, :] + total
            moved = acc_in[here, :] + moved
        if last:
            rowsum = jnp.sum(total, axis=1, keepdims=True)
            diff = (2.0 / lsq_ref[0]) * (moved - rowsum * rf[here, :].astype(jnp.float32))
            for b in range(ROW_CHUNK // PTS):
                side, block = divmod(r * (ROW_CHUNK // PTS) + b, out_ref.shape[1])
                out_ref[side, block] = diff[b * PTS : (b + 1) * PTS, :].astype(jnp.bfloat16)
        else:
            rs[here, :] = total
            acc[here, :] = moved


def chunk(sums, prepared, cols, amp, lsq, last):
    rf, la, ai = prepared
    r = rf.shape[0]
    c = len(cols) * PTS
    first = sums is None
    sums_shape = (
        jax.ShapeDtypeStruct((r, FEAT), jnp.float32),
        jax.ShapeDtypeStruct((r, 128), jnp.float32),
    )
    scratch = [pltpu.VMEM((c, FEAT), jnp.bfloat16), pltpu.VMEM((128, c), jnp.bfloat16)]
    if last:
        out_shape = jax.ShapeDtypeStruct((2, r // PTS // 2, PTS, FEAT), jnp.bfloat16)
        out_specs = VMEM
        scratch += [pltpu.VMEM((8, 128), jnp.float32), pltpu.VMEM((8, 128), jnp.float32)]
    else:
        out_shape, out_specs = sums_shape, (VMEM, VMEM)
    operands = (amp, lsq, rf, la, ai) + (() if first else tuple(sums)) + tuple(cols)
    return pl.pallas_call(
        functools.partial(chunk_kernel, len(cols), first, last),
        out_shape=out_shape,
        in_specs=[SMEM, SMEM] + [VMEM] * (len(operands) - 2),
        out_specs=out_specs,
        scratch_shapes=scratch,
        cost_estimate=pl.CostEstimate(
            flops=2 * r * c * 1280, bytes_accessed=4 * r * FEAT, transcendentals=r * c
        ),
        compiler_params=pltpu.CompilerParams(vmem_limit_bytes=16 * 1024 * 1024),
        name="chunk",
    )(*operands)


def message_kernel(hidden_ref, proj_ref, alpha_ref, probes_ref, out_ref):
    feats = jnp.dot(hidden_ref[...], proj_ref[...], preferred_element_type=jnp.float32).astype(
        jnp.bfloat16
    )
    feat_f = feats.astype(jnp.float32)
    for k in range(4):
        out_ref[k * 128 : (k + 1) * 128, :] = feats[:, k * 128 : (k + 1) * 128]
    sq = jnp.sum(feat_f * feat_f, axis=1, keepdims=True)
    hi = sq.astype(jnp.bfloat16).astype(jnp.float32)
    mid = (sq - hi).astype(jnp.bfloat16).astype(jnp.float32)
    low = sq - hi - mid
    probes = probes_ref[...].astype(jnp.float32)
    wide = jnp.concatenate([probes, hi, mid, low, jnp.zeros((PTS, 93), jnp.float32)], axis=1).T
    fac = jnp.concatenate([alpha_ref[...].astype(jnp.float32), wide[0:47]], axis=0)
    out_ref[FEAT:MSG, :] = fac.astype(jnp.bfloat16)


def message(hidden, projection, alpha, probe_pairs):
    return pl.pallas_call(
        message_kernel,
        out_shape=jax.ShapeDtypeStruct((MSG, 128), jnp.bfloat16),
        in_specs=[VMEM] * 4,
        out_specs=VMEM,
        name="message",
    )(hidden, projection, alpha.reshape(1, PTS), probe_pairs)


def sent_to_all(x, axes, size):
    return lax.all_to_all(jnp.broadcast_to(x[None], (size, *x.shape)), axes, 0, 0, tiled=True)


def shifted(x, axis, by):
    n = lax.axis_size(axis)
    return lax.ppermute(x, axis, [(i, (i + by) % n) for i in range(n)])


def steps(hidden, projection, alpha, probe_pairs, amplitude, length_sq):
    msg = message(hidden, projection, alpha, probe_pairs)
    rows = sent_to_all(msg, ("x", "yl"), 8)
    prepared = prepare(rows, shifted(rows, "c", 1), length_sq)
    across = shifted(msg, "yh", 1)
    order = [msg, across]
    ups, downs = [msg, across], [msg, across]
    for k in range(1, 5):
        for chain in range(2):
            ups[chain] = shifted(ups[chain], "z", 1)
            order.append(ups[chain])
            if k < 4:
                downs[chain] = shifted(downs[chain], "z", -1)
                order.append(downs[chain])
    sums = None
    for k in range(4):
        sums = chunk(sums, prepared, order[4 * k : 4 * k + 4], amplitude, length_sq, k == 3)
    part = sums[0] + shifted(sums[1], "c", 1)
    arrived = lax.all_to_all(part, ("x", "yl"), 0, 0, tiled=True)
    grad_feat = arrived.astype(jnp.float32).sum(axis=0).astype(jnp.bfloat16)
    grad_hidden = jnp.dot(grad_feat, projection.T, preferred_element_type=jnp.float32).astype(
        jnp.bfloat16
    )
    partial = lax.dot_general(
        hidden, grad_feat, (((0,), (0,)), ((), ())), preferred_element_type=jnp.float32
    ).astype(jnp.bfloat16)
    blocks = partial.reshape(2, 8, 2, 24, FEAT).transpose(2, 1, 0, 3, 4)
    got = lax.all_to_all(blocks, "c", 0, 0, tiled=True)
    core_sum = got.astype(jnp.float32).sum(axis=0).astype(jnp.bfloat16)
    got = lax.all_to_all(core_sum, "z", 0, 0, tiled=True)
    z_sum = got.astype(jnp.float32).sum(axis=0).astype(jnp.bfloat16)
    spread = jnp.broadcast_to(z_sum[:, None], (2, 8, 24, FEAT)).reshape(16, 24, FEAT)
    got = lax.all_to_all(spread, ("yh", "x", "yl"), 0, 0, tiled=True)
    grad_proj = got.astype(jnp.float32).sum(axis=0)
    return grad_hidden, grad_proj


def solution(mesh):
    fine = Mesh(mesh.devices.reshape(2, 8, 2, 4, 2), ALL)
    placed = (P(ALL, None), P(), P(ALL), P(ALL, None), P(), P())
    return jax.shard_map(
        steps,
        mesh=fine,
        in_specs=placed,
        out_specs=(P(ALL, None), P(("yh", "z", "c"), None)),
        check_vma=False,
    )
```

```python
import functools

import jax
import jax.numpy as jnp
from jax import lax
from jax.experimental import pallas as pl
from jax.experimental.pallas import tpu as pltpu
from jax.sharding import Mesh, PartitionSpec as P


LOG2E = 1.4426950408889634
PTS = 128
FEAT = 512
HID = 768
ROW_MSG = 816
MSG = 560
ROW_CHUNK = 512
ALL = ("yh", "z", "c", "x", "yl")
VMEM = pl.BlockSpec(memory_space=pltpu.VMEM)
SMEM = pl.BlockSpec(memory_space=pltpu.SMEM)


def prepare_kernel(n, lsq_ref, proj_ref, *refs):
    bundles, (hr, rf, la, ai) = refs[: 2 * n], refs[2 * n :]
    half = 0.5 * LOG2E / lsq_ref[0]
    lane = lax.broadcasted_iota(jnp.int32, (PTS, 128), 1)
    for side in range(2):
        for dx in range(n):
            ref = bundles[side * n + dx]
            for dy in range(2):
                at = ((side * n + dx) * 2 + dy) * PTS
                here = slice(at, at + PTS)
                base = dy * ROW_MSG
                for k in range(6):
                    hr[here, k * 128 : (k + 1) * 128] = ref[
                        base + k * 128 : base + (k + 1) * 128, :
                    ]
                fac = ref[base + HID : base + ROW_MSG, :].astype(jnp.float32)
                sq = fac[33:34] + fac[34:35] + fac[35:36]
                swapped = jnp.concatenate(
                    [
                        fac[0:1] * 0.5,
                        fac[17:33] * (-1 / 64),
                        fac[1:17] * (-1 / 64),
                        sq * half,
                        jnp.zeros((94, 128), jnp.float32),
                    ],
                    axis=0,
                ).T
                ai[here, :] = jnp.broadcast_to(swapped[:, 33:34], (PTS, 128))
                la[here, :] = jnp.where(lane < 33, swapped, 0.0).astype(jnp.bfloat16)
    for r in range(rf.shape[0] // ROW_CHUNK):
        here = slice(r * ROW_CHUNK, (r + 1) * ROW_CHUNK)
        rf[here, :] = jnp.dot(
            hr[here, :], proj_ref[...], preferred_element_type=jnp.float32
        ).astype(jnp.bfloat16)


def prepare(near, far, projection, lsq):
    n = len(near)
    r = 4 * n * PTS
    return pl.pallas_call(
        functools.partial(prepare_kernel, n),
        out_shape=(
            jax.ShapeDtypeStruct((r, HID), jnp.bfloat16),
            jax.ShapeDtypeStruct((r, FEAT), jnp.bfloat16),
            jax.ShapeDtypeStruct((r, 128), jnp.bfloat16),
            jax.ShapeDtypeStruct((r, 128), jnp.float32),
        ),
        in_specs=[SMEM, VMEM] + [VMEM] * (2 * n),
        out_specs=(VMEM,) * 4,
        cost_estimate=pl.CostEstimate(
            flops=2 * r * HID * FEAT, bytes_accessed=r * FEAT, transcendentals=0
        ),
        compiler_params=pltpu.CompilerParams(vmem_limit_bytes=10 * 1024 * 1024),
        name="prepare",
    )(lsq, projection, *near, *far)


def chunk_kernel(n, first, last, amp_ref, lsq_ref, rf, la, ai, *refs):
    if not first:
        acc_in, rs_in = refs[:2]
        refs = refs[2:]
    cols_refs = refs[:n]
    refs = refs[n:]
    if last:
        out_ref, cf, cfac, acc, rs = refs
    else:
        acc, rs, cf, cfac = refs
    rows, width = rf.shape[0], cf.shape[0]
    c1 = LOG2E / lsq_ref[0]
    half = 0.5 * c1
    at = 0
    for ref in cols_refs:
        for base in range(0, ref.shape[0], MSG):
            for k in range(4):
                cf[at : at + PTS, k * 128 : (k + 1) * 128] = ref[
                    base + k * 128 : base + (k + 1) * 128, :
                ]
            cfac[0:48, at : at + PTS] = ref[base + FEAT : base + MSG, :]
            at += PTS
    cfac[48:, :] = jnp.zeros((80, width), jnp.bfloat16)
    f3 = cfac[32:40, :].astype(jnp.float32)
    bj = (f3[1:2] + f3[2:3] + f3[3:4]) * half - jnp.log2(
        jnp.full((1, width), amp_ref[0], jnp.float32)
    )
    for r in range(rows // ROW_CHUNK):
        here = slice(r * ROW_CHUNK, (r + 1) * ROW_CHUNK)
        inner = lax.dot_general(
            rf[here, :], cf[...], (((1,), (1,)), ((), ())), preferred_element_type=jnp.float32
        )
        gmat = jnp.dot(la[here, :], cfac[...], preferred_element_type=jnp.float32)
        a = jnp.concatenate([ai[here, :]] * (width // 128), axis=1)
        w = gmat * jnp.exp2(inner * c1 - a - bj)
        total = w[:, 0:128]
        for q in range(1, width // 128):
            total = total + w[:, q * 128 : (q + 1) * 128]
        moved = jnp.dot(w.astype(jnp.bfloat16), cf[...], preferred_element_type=jnp.float32)
        if not first:
            total = rs_in[here, :] + total
            moved = acc_in[here, :] + moved
        if last:
            rowsum = jnp.sum(total, axis=1, keepdims=True)
            diff = (2.0 / lsq_ref[0]) * (moved - rowsum * rf[here, :].astype(jnp.float32))
            for b in range(ROW_CHUNK // PTS):
                side, block = divmod(r * (ROW_CHUNK // PTS) + b, out_ref.shape[1])
                out_ref[side, block] = diff[b * PTS : (b + 1) * PTS, :].astype(jnp.bfloat16)
        else:
            rs[here, :] = total
            acc[here, :] = moved


def chunk(sums, prepared, cols, amp, lsq, last):
    rf, la, ai = prepared
    r = rf.shape[0]
    c = sum(x.shape[0] for x in cols) // MSG * PTS
    first = sums is None
    sums_shape = (
        jax.ShapeDtypeStruct((r, FEAT), jnp.float32),
        jax.ShapeDtypeStruct((r, 128), jnp.float32),
    )
    scratch = [pltpu.VMEM((c, FEAT), jnp.bfloat16), pltpu.VMEM((128, c), jnp.bfloat16)]
    if last:
        out_shape = jax.ShapeDtypeStruct((2, r // PTS // 2, PTS, FEAT), jnp.bfloat16)
        out_specs = VMEM
        scratch += [pltpu.VMEM((8, 128), jnp.float32), pltpu.VMEM((8, 128), jnp.float32)]
    else:
        out_shape, out_specs = sums_shape, (VMEM, VMEM)
    operands = (amp, lsq, rf, la, ai) + (() if first else tuple(sums)) + tuple(cols)
    return pl.pallas_call(
        functools.partial(chunk_kernel, len(cols), first, last),
        out_shape=out_shape,
        in_specs=[SMEM, SMEM] + [VMEM] * (len(operands) - 2),
        out_specs=out_specs,
        scratch_shapes=scratch,
        cost_estimate=pl.CostEstimate(
            flops=2 * r * c * 1280, bytes_accessed=4 * r * FEAT, transcendentals=r * c
        ),
        compiler_params=pltpu.CompilerParams(vmem_limit_bytes=10 * 1024 * 1024),
        name="chunk",
    )(*operands)


def message_kernel(hidden_ref, proj_ref, alpha_ref, probes_ref, out_ref, row_ref):
    feats = jnp.dot(hidden_ref[...], proj_ref[...], preferred_element_type=jnp.float32).astype(
        jnp.bfloat16
    )
    feat_f = feats.astype(jnp.float32)
    for k in range(4):
        out_ref[k * 128 : (k + 1) * 128, :] = feats[:, k * 128 : (k + 1) * 128]
    sq = jnp.sum(feat_f * feat_f, axis=1, keepdims=True)
    hi = sq.astype(jnp.bfloat16).astype(jnp.float32)
    mid = (sq - hi).astype(jnp.bfloat16).astype(jnp.float32)
    low = sq - hi - mid
    probes = probes_ref[...].astype(jnp.float32)
    wide = jnp.concatenate([probes, hi, mid, low, jnp.zeros((PTS, 93), jnp.float32)], axis=1).T
    fac = jnp.concatenate([alpha_ref[...].astype(jnp.float32), wide[0:47]], axis=0)
    out_ref[FEAT:MSG, :] = fac.astype(jnp.bfloat16)
    for k in range(6):
        row_ref[k * 128 : (k + 1) * 128, :] = hidden_ref[:, k * 128 : (k + 1) * 128]
    row_ref[HID:ROW_MSG, :] = fac.astype(jnp.bfloat16)


def message(hidden, projection, alpha, probe_pairs):
    return pl.pallas_call(
        message_kernel,
        out_shape=(
            jax.ShapeDtypeStruct((MSG, 128), jnp.bfloat16),
            jax.ShapeDtypeStruct((ROW_MSG, 128), jnp.bfloat16),
        ),
        in_specs=[VMEM] * 4,
        out_specs=(VMEM, VMEM),
        name="message",
    )(hidden, projection, alpha.reshape(1, PTS), probe_pairs)


def shifted(x, axis, by):
    n = lax.axis_size(axis)
    return lax.ppermute(x, axis, [(i, (i + by) % n) for i in range(n)])


def apart(x):
    n = lax.axis_size("z")
    hops = [(2 * i + c, 2 * ((i + (1, -1)[c]) % n) + c) for i in range(n) for c in range(2)]
    return lax.ppermute(x, ("z", "c"), hops)


def steps(hidden, projection, alpha, probe_pairs, amplitude, length_sq):
    msg, row_msg = message(hidden, projection, alpha, probe_pairs)
    pair_rows = jnp.concatenate([row_msg, shifted(row_msg, "yl", 1)], axis=0)
    near = [pair_rows] + [shifted(pair_rows, "x", k) for k in (1, 2, 3)]
    far = [shifted(b, "c", 1) for b in near]
    hidden_rows, *prepared = prepare(near, far, projection, length_sq)
    own = jnp.concatenate([msg, shifted(msg, "yh", 1)], axis=0)
    held = jnp.concatenate([own, shifted(own, "c", 1)], axis=0)
    ring = []
    for k in range(1, 5):
        held = apart(held if k < 4 else held[: 2 * MSG])
        ring.append(held)
    groups = [[own, ring[0]], ring[1:2], ring[2:3], ring[3:4]]
    sums = None
    for k, group in enumerate(groups):
        sums = chunk(sums, prepared, group, amplitude, length_sq, k == 3)
    partial = lax.dot_general(
        hidden_rows,
        sums.reshape(hidden_rows.shape[0], FEAT),
        (((0,), (0,)), ((), ())),
        preferred_element_type=jnp.float32,
    ).astype(jnp.bfloat16)
    part = sums[0] + shifted(sums[1], "c", 1)
    total = part[0:2].astype(jnp.float32)
    for k in (1, 2, 3):
        total = total + shifted(part[2 * k : 2 * k + 2], "x", -k).astype(jnp.float32)
    aside = shifted(total[1].astype(jnp.bfloat16), "yl", 1)
    grad_feat = (total[0] + aside.astype(jnp.float32)).astype(jnp.bfloat16)
    grad_hidden = jnp.dot(grad_feat, projection.T, preferred_element_type=jnp.float32).astype(
        jnp.bfloat16
    )
    blocks = partial.reshape(2, 8, 2, 24, FEAT).transpose(2, 1, 0, 3, 4)
    core = lax.axis_index("c")
    mine = lax.dynamic_index_in_dim(blocks, core, 0, keepdims=False)
    other = lax.dynamic_index_in_dim(blocks, 1 - core, 0, keepdims=False)
    core_sum = mine + shifted(other, "c", 1)
    got = lax.all_to_all(core_sum, "z", 0, 0, tiled=True)
    z_sum = got.astype(jnp.float32).sum(axis=0).astype(jnp.bfloat16)
    spread = jnp.broadcast_to(z_sum[:, None], (2, 8, 24, FEAT)).reshape(16, 24, FEAT)
    got = lax.all_to_all(spread, ("yh", "x", "yl"), 0, 0, tiled=True)
    grad_proj = got.astype(jnp.float32).sum(axis=0)
    return grad_hidden, grad_proj


def solution(mesh):
    fine = Mesh(mesh.devices.reshape(2, 8, 2, 4, 2), ALL)
    placed = (P(ALL, None), P(), P(ALL), P(ALL, None), P(), P())
    return jax.shard_map(
        steps,
        mesh=fine,
        in_specs=placed,
        out_specs=(P(ALL, None), P(("yh", "z", "c"), None)),
        check_vma=False,
    )
```

```python
import functools

import jax
import jax.numpy as jnp
from jax import lax
from jax.experimental import pallas as pl
from jax.experimental.pallas import tpu as pltpu
from jax.sharding import Mesh, PartitionSpec as P


LOG2E = 1.4426950408889634
PTS = 128
FEAT = 512
HID = 768
ROW_MSG = 816
MSG = 560
ROW_CHUNK = 512
ALL = ("yh", "z", "c", "x", "yl")
VMEM = pl.BlockSpec(memory_space=pltpu.VMEM)
SMEM = pl.BlockSpec(memory_space=pltpu.SMEM)


def prepare_kernel(n, lsq_ref, proj_ref, *refs):
    bundles, (hr, rf, la, ai) = refs[:n], refs[n:]
    half = 0.5 * LOG2E / lsq_ref[0]
    lane = lax.broadcasted_iota(jnp.int32, (PTS, 128), 1)
    for dx in range(n):
        ref = bundles[dx]
        for dy in range(2):
            at = (dx * 2 + dy) * PTS
            here = slice(at, at + PTS)
            base = dy * ROW_MSG
            for k in range(6):
                hr[here, k * 128 : (k + 1) * 128] = ref[base + k * 128 : base + (k + 1) * 128, :]
            fac = ref[base + HID : base + ROW_MSG, :].astype(jnp.float32)
            sq = fac[33:34] + fac[34:35] + fac[35:36]
            swapped = jnp.concatenate(
                [
                    fac[0:1] * 0.5,
                    fac[17:33] * (-1 / 64),
                    fac[1:17] * (-1 / 64),
                    sq * half,
                    jnp.zeros((94, 128), jnp.float32),
                ],
                axis=0,
            ).T
            ai[here, :] = jnp.broadcast_to(swapped[:, 33:34], (PTS, 128))
            la[here, :] = jnp.where(lane < 33, swapped, 0.0).astype(jnp.bfloat16)
    for r in range(rf.shape[0] // ROW_CHUNK):
        here = slice(r * ROW_CHUNK, (r + 1) * ROW_CHUNK)
        rf[here, :] = jnp.dot(
            hr[here, :], proj_ref[...], preferred_element_type=jnp.float32
        ).astype(jnp.bfloat16)


def prepare(bundles, projection, lsq):
    n = len(bundles)
    r = 2 * n * PTS
    return pl.pallas_call(
        functools.partial(prepare_kernel, n),
        out_shape=(
            jax.ShapeDtypeStruct((r, HID), jnp.bfloat16),
            jax.ShapeDtypeStruct((r, FEAT), jnp.bfloat16),
            jax.ShapeDtypeStruct((r, 128), jnp.bfloat16),
            jax.ShapeDtypeStruct((r, 128), jnp.float32),
        ),
        in_specs=[SMEM, VMEM] + [VMEM] * n,
        out_specs=(VMEM,) * 4,
        cost_estimate=pl.CostEstimate(
            flops=2 * r * HID * FEAT, bytes_accessed=r * FEAT, transcendentals=0
        ),
        compiler_params=pltpu.CompilerParams(vmem_limit_bytes=10 * 1024 * 1024),
        name="prepare",
    )(lsq, projection, *bundles)


def chunk_kernel(n, first, last, amp_ref, lsq_ref, *refs):
    sides, refs = (refs[0:3], refs[3:6]), refs[6:]
    if not first:
        acc_in, rs_in = refs[:2]
        refs = refs[2:]
    cols_refs = refs[:n]
    refs = refs[n:]
    if last:
        near_ref, far_ref, cf, cfac = refs
    else:
        acc, rs, cf, cfac = refs
    rows, width = sides[0][0].shape[0], cf.shape[0]
    c1 = LOG2E / lsq_ref[0]
    half = 0.5 * c1
    at = 0
    for ref in cols_refs:
        for base in range(0, ref.shape[0], MSG):
            for k in range(4):
                cf[at : at + PTS, k * 128 : (k + 1) * 128] = ref[
                    base + k * 128 : base + (k + 1) * 128, :
                ]
            cfac[0:48, at : at + PTS] = ref[base + FEAT : base + MSG, :]
            at += PTS
    cfac[48:, :] = jnp.zeros((80, width), jnp.bfloat16)
    f3 = cfac[32:40, :].astype(jnp.float32)
    bj = (f3[1:2] + f3[2:3] + f3[3:4]) * half - jnp.log2(
        jnp.full((1, width), amp_ref[0], jnp.float32)
    )
    for r in range(2 * rows // ROW_CHUNK):
        here = slice(r * ROW_CHUNK, (r + 1) * ROW_CHUNK)
        side, inside = divmod(r * ROW_CHUNK, rows)
        local = slice(inside, inside + ROW_CHUNK)
        rf, la, ai = sides[side]
        inner = lax.dot_general(
            rf[local, :], cf[...], (((1,), (1,)), ((), ())), preferred_element_type=jnp.float32
        )
        gmat = jnp.dot(la[local, :], cfac[...], preferred_element_type=jnp.float32)
        a = jnp.concatenate([ai[local, :]] * (width // 128), axis=1)
        w = gmat * jnp.exp2(inner * c1 - a - bj)
        total = w[:, 0:128]
        for q in range(1, width // 128):
            total = total + w[:, q * 128 : (q + 1) * 128]
        moved = jnp.dot(w.astype(jnp.bfloat16), cf[...], preferred_element_type=jnp.float32)
        if not first:
            total = rs_in[here, :] + total
            moved = acc_in[here, :] + moved
        if last:
            rowsum = jnp.sum(total, axis=1, keepdims=True)
            diff = (2.0 / lsq_ref[0]) * (moved - rowsum * rf[local, :].astype(jnp.float32))
            (near_ref, far_ref)[side][local, :] = diff.astype(jnp.bfloat16)
        else:
            rs[here, :] = total
            acc[here, :] = moved


def chunk(sums, prepared, cols, amp, lsq, last):
    r = 2 * prepared[0].shape[0]
    c = sum(x.shape[0] for x in cols) // MSG * PTS
    first = sums is None
    sums_shape = (
        jax.ShapeDtypeStruct((r, FEAT), jnp.float32),
        jax.ShapeDtypeStruct((r, 128), jnp.float32),
    )
    scratch = [pltpu.VMEM((c, FEAT), jnp.bfloat16), pltpu.VMEM((128, c), jnp.bfloat16)]
    if last:
        out_shape, out_specs = (jax.ShapeDtypeStruct((r // 2, FEAT), jnp.bfloat16),) * 2, (VMEM, VMEM)
    else:
        out_shape, out_specs = sums_shape, (VMEM, VMEM)
    operands = (amp, lsq, *prepared) + (() if first else tuple(sums)) + tuple(cols)
    return pl.pallas_call(
        functools.partial(chunk_kernel, len(cols), first, last),
        out_shape=out_shape,
        in_specs=[SMEM, SMEM] + [VMEM] * (len(operands) - 2),
        out_specs=out_specs,
        scratch_shapes=scratch,
        cost_estimate=pl.CostEstimate(
            flops=2 * r * c * 1280, bytes_accessed=4 * r * FEAT, transcendentals=r * c
        ),
        compiler_params=pltpu.CompilerParams(vmem_limit_bytes=10 * 1024 * 1024),
        name="chunk",
    )(*operands)


def message_kernel(hidden_ref, proj_ref, alpha_ref, probes_ref, out_ref, row_ref):
    feats = jnp.dot(hidden_ref[...], proj_ref[...], preferred_element_type=jnp.float32).astype(
        jnp.bfloat16
    )
    feat_f = feats.astype(jnp.float32)
    for k in range(4):
        out_ref[k * 128 : (k + 1) * 128, :] = feats[:, k * 128 : (k + 1) * 128]
    sq = jnp.sum(feat_f * feat_f, axis=1, keepdims=True)
    hi = sq.astype(jnp.bfloat16).astype(jnp.float32)
    mid = (sq - hi).astype(jnp.bfloat16).astype(jnp.float32)
    low = sq - hi - mid
    wide = jnp.concatenate([hi, mid, low, jnp.zeros((PTS, 125), jnp.float32)], axis=1).T
    fac = jnp.concatenate(
        [alpha_ref[...].astype(jnp.float32), probes_ref[...].astype(jnp.float32), wide[0:15]],
        axis=0,
    )
    out_ref[FEAT:MSG, :] = fac.astype(jnp.bfloat16)
    for k in range(6):
        row_ref[k * 128 : (k + 1) * 128, :] = hidden_ref[:, k * 128 : (k + 1) * 128]
    row_ref[HID:ROW_MSG, :] = fac.astype(jnp.bfloat16)


def message(hidden, projection, alpha, probe_pairs):
    return pl.pallas_call(
        message_kernel,
        out_shape=(
            jax.ShapeDtypeStruct((MSG, 128), jnp.bfloat16),
            jax.ShapeDtypeStruct((ROW_MSG, 128), jnp.bfloat16),
        ),
        in_specs=[VMEM] * 4,
        out_specs=(VMEM, VMEM),
        name="message",
    )(hidden, projection, alpha.reshape(1, PTS), probe_pairs.T)


def halve_kernel(partial_ref, mine_ref, other_ref):
    first = lax.axis_index("c") == 0
    for yh in range(2):
        for z in range(8):
            at = (yh * 8 + z) * 48
            a, b = partial_ref[at : at + 24, :], partial_ref[at + 24 : at + 48, :]
            mine_ref[z, yh] = jnp.where(first, a, b)
            other_ref[z, yh] = jnp.where(first, b, a)


def halve(partial):
    half = jax.ShapeDtypeStruct((8, 2, 24, FEAT), jnp.bfloat16)
    return pl.pallas_call(
        halve_kernel,
        out_shape=(half, half),
        in_specs=[VMEM],
        out_specs=(VMEM, VMEM),
        compiler_params=pltpu.CompilerParams(vmem_limit_bytes=10 * 1024 * 1024),
        name="halve",
    )(partial)


def spread_kernel(got_ref, out_ref):
    for yh in range(2):
        total = got_ref[0, yh].astype(jnp.float32)
        for z in range(1, 8):
            total = total + got_ref[z, yh].astype(jnp.float32)
        for k in range(8):
            out_ref[yh * 8 + k] = total.astype(jnp.bfloat16)


def spread(got):
    return pl.pallas_call(
        spread_kernel,
        out_shape=jax.ShapeDtypeStruct((16, 24, FEAT), jnp.bfloat16),
        in_specs=[VMEM],
        out_specs=VMEM,
        compiler_params=pltpu.CompilerParams(vmem_limit_bytes=10 * 1024 * 1024),
        name="spread",
    )(got)


def shifted(x, axis, by):
    n = lax.axis_size(axis)
    return lax.ppermute(x, axis, [(i, (i + by) % n) for i in range(n)])


def apart(x):
    n = lax.axis_size("z")
    hops = [(2 * i + c, 2 * ((i + (1, -1)[c]) % n) + c) for i in range(n) for c in range(2)]
    return lax.ppermute(x, ("z", "c"), hops)


def steps(hidden, projection, alpha, probe_pairs, amplitude, length_sq):
    msg, row_msg = message(hidden, projection, alpha, probe_pairs)
    pair_rows = jnp.concatenate([row_msg, shifted(row_msg, "yl", 1)], axis=0)
    near = [pair_rows] + [shifted(pair_rows, "x", k) for k in (1, 2, 3)]
    far = [shifted(b, "c", 1) for b in near]
    hidden_near, *prepared = prepare(near, projection, length_sq)
    hidden_far, *more = prepare(far, projection, length_sq)
    prepared += more
    ring = [jnp.concatenate([msg, shifted(msg, "c", 1)], axis=0)]
    for k in range(1, 5):
        ring.append(apart(ring[-1] if k < 4 else ring[-1][:MSG]))
    crossed = [shifted(b, "yh", 1) for b in [msg] + ring[1:]]
    groups = [[msg, ring[1], crossed[0]], ring[2:4], crossed[1:3], [ring[4]] + crossed[3:5]]
    sums = None
    for k, group in enumerate(groups):
        sums = chunk(sums, prepared, group, amplitude, length_sq, k == 3)
    near_diff, far_diff = sums
    across_rows = (((0,), (0,)), ((), ()))
    partial = lax.dot_general(
        hidden_near, near_diff, across_rows, preferred_element_type=jnp.float32
    )
    partial += lax.dot_general(
        hidden_far, far_diff, across_rows, preferred_element_type=jnp.float32
    )
    partial = partial.astype(jnp.bfloat16)
    part = (near_diff + shifted(far_diff, "c", 1)).reshape(8, PTS, FEAT)
    owned = [shifted(part[2 * k : 2 * k + 2], "x", -k) for k in (1, 2, 3)]
    total = part[0:2].astype(jnp.float32)
    for piece in owned:
        total = total + piece.astype(jnp.float32)
    aside = shifted(total[1].astype(jnp.bfloat16), "yl", 1)
    grad_feat = (total[0] + aside.astype(jnp.float32)).astype(jnp.bfloat16)
    grad_hidden = jnp.dot(grad_feat, projection.T, preferred_element_type=jnp.float32).astype(
        jnp.bfloat16
    )
    mine, other = halve(partial)
    core_sum = mine + shifted(other, "c", 1)
    got = lax.all_to_all(core_sum, "z", 0, 0, tiled=True)
    got = lax.all_to_all(spread(got), ("yh", "x", "yl"), 0, 0, tiled=True)
    grad_proj = got.astype(jnp.float32).sum(axis=0)
    return grad_hidden, grad_proj


def solution(mesh):
    fine = Mesh(mesh.devices.reshape(2, 8, 2, 4, 2), ALL)
    placed = (P(ALL, None), P(), P(ALL), P(ALL, None), P(), P())
    return jax.shard_map(
        steps,
        mesh=fine,
        in_specs=placed,
        out_specs=(P(ALL, None), P(("yh", "z", "c"), None)),
        check_vma=False,
    )
```

```python
import functools

import jax
import jax.numpy as jnp
from jax import lax
from jax.experimental import pallas as pl
from jax.experimental.pallas import tpu as pltpu
from jax.sharding import Mesh, PartitionSpec as P


LOG2E = 1.4426950408889634
PTS = 128
FEAT = 512
HID = 768
ROW_MSG = 816
MSG = 560
ROW_CHUNK = 512
ALL = ("yh", "z", "c", "x", "yl")
VMEM = pl.BlockSpec(memory_space=pltpu.VMEM)
SMEM = pl.BlockSpec(memory_space=pltpu.SMEM)


def prepare_kernel(n, lsq_ref, proj_ref, *refs):
    bundles, (hr, rf, la, ai) = refs[:n], refs[n:]
    half = 0.5 * LOG2E / lsq_ref[0]
    lane = lax.broadcasted_iota(jnp.int32, (PTS, 128), 1)
    for dx in range(n):
        ref = bundles[dx]
        for dy in range(2):
            at = (dx * 2 + dy) * PTS
            here = slice(at, at + PTS)
            base = dy * ROW_MSG
            for k in range(6):
                hr[here, k * 128 : (k + 1) * 128] = ref[base + k * 128 : base + (k + 1) * 128, :]
            fac = ref[base + HID : base + ROW_MSG, :].astype(jnp.float32)
            sq = fac[33:34] + fac[34:35] + fac[35:36]
            swapped = jnp.concatenate(
                [
                    fac[0:1] * 0.5,
                    fac[17:33] * (-1 / 64),
                    fac[1:17] * (-1 / 64),
                    sq * half,
                    jnp.zeros((94, 128), jnp.float32),
                ],
                axis=0,
            ).T
            ai[here, :] = jnp.broadcast_to(swapped[:, 33:34], (PTS, 128))
            la[here, :] = jnp.where(lane < 33, swapped, 0.0).astype(jnp.bfloat16)
    for r in range(rf.shape[0] // ROW_CHUNK):
        here = slice(r * ROW_CHUNK, (r + 1) * ROW_CHUNK)
        rf[here, :] = jnp.dot(
            hr[here, :], proj_ref[...], preferred_element_type=jnp.float32
        ).astype(jnp.bfloat16)


def prepare(bundles, projection, lsq):
    n = len(bundles)
    r = 2 * n * PTS
    return pl.pallas_call(
        functools.partial(prepare_kernel, n),
        out_shape=(
            jax.ShapeDtypeStruct((r, HID), jnp.bfloat16),
            jax.ShapeDtypeStruct((r, FEAT), jnp.bfloat16),
            jax.ShapeDtypeStruct((r, 128), jnp.bfloat16),
            jax.ShapeDtypeStruct((r, 128), jnp.float32),
        ),
        in_specs=[SMEM, VMEM] + [VMEM] * n,
        out_specs=(VMEM,) * 4,
        cost_estimate=pl.CostEstimate(
            flops=2 * r * HID * FEAT, bytes_accessed=r * FEAT, transcendentals=0
        ),
        compiler_params=pltpu.CompilerParams(vmem_limit_bytes=10 * 1024 * 1024),
        name="prepare",
    )(lsq, projection, *bundles)


def chunk_kernel(n, first, last, amp_ref, lsq_ref, *refs):
    sides, refs = (refs[0:3], refs[3:6]), refs[6:]
    if not first:
        acc_in, rs_in = refs[:2]
        refs = refs[2:]
    cols_refs = refs[:n]
    refs = refs[n:]
    if last:
        near_ref, far_ref, cf, cfac = refs
    else:
        acc, rs, cf, cfac = refs
    rows, width = sides[0][0].shape[0], cf.shape[0]
    c1 = LOG2E / lsq_ref[0]
    half = 0.5 * c1
    at = 0
    for ref in cols_refs:
        for base in range(0, ref.shape[0], MSG):
            for k in range(4):
                cf[at : at + PTS, k * 128 : (k + 1) * 128] = ref[
                    base + k * 128 : base + (k + 1) * 128, :
                ]
            cfac[0:48, at : at + PTS] = ref[base + FEAT : base + MSG, :]
            at += PTS
    cfac[48:, :] = jnp.zeros((80, width), jnp.bfloat16)
    f3 = cfac[32:40, :].astype(jnp.float32)
    bj = (f3[1:2] + f3[2:3] + f3[3:4]) * half - jnp.log2(
        jnp.full((1, width), amp_ref[0], jnp.float32)
    )
    for r in range(2 * rows // ROW_CHUNK):
        here = slice(r * ROW_CHUNK, (r + 1) * ROW_CHUNK)
        side, inside = divmod(r * ROW_CHUNK, rows)
        local = slice(inside, inside + ROW_CHUNK)
        rf, la, ai = sides[side]
        inner = lax.dot_general(
            rf[local, :], cf[...], (((1,), (1,)), ((), ())), preferred_element_type=jnp.float32
        )
        gmat = jnp.dot(la[local, :], cfac[...], preferred_element_type=jnp.float32)
        a = jnp.concatenate([ai[local, :]] * (width // 128), axis=1)
        w = gmat * jnp.exp2(inner * c1 - a - bj)
        total = w[:, 0:128]
        for q in range(1, width // 128):
            total = total + w[:, q * 128 : (q + 1) * 128]
        moved = jnp.dot(w.astype(jnp.bfloat16), cf[...], preferred_element_type=jnp.float32)
        if not first:
            total = rs_in[here, :] + total
            moved = acc_in[here, :] + moved
        if last:
            rowsum = jnp.sum(total, axis=1, keepdims=True)
            diff = (2.0 / lsq_ref[0]) * (moved - rowsum * rf[local, :].astype(jnp.float32))
            (near_ref, far_ref)[side][local, :] = diff.astype(jnp.bfloat16)
        else:
            rs[here, :] = total
            acc[here, :] = moved


def chunk(sums, prepared, cols, amp, lsq, last):
    r = 2 * prepared[0].shape[0]
    c = sum(x.shape[0] for x in cols) // MSG * PTS
    first = sums is None
    sums_shape = (
        jax.ShapeDtypeStruct((r, FEAT), jnp.float32),
        jax.ShapeDtypeStruct((r, 128), jnp.float32),
    )
    scratch = [pltpu.VMEM((c, FEAT), jnp.bfloat16), pltpu.VMEM((128, c), jnp.bfloat16)]
    if last:
        out_shape, out_specs = (jax.ShapeDtypeStruct((r // 2, FEAT), jnp.bfloat16),) * 2, (VMEM, VMEM)
    else:
        out_shape, out_specs = sums_shape, (VMEM, VMEM)
    operands = (amp, lsq, *prepared) + (() if first else tuple(sums)) + tuple(cols)
    return pl.pallas_call(
        functools.partial(chunk_kernel, len(cols), first, last),
        out_shape=out_shape,
        in_specs=[SMEM, SMEM] + [VMEM] * (len(operands) - 2),
        out_specs=out_specs,
        scratch_shapes=scratch,
        cost_estimate=pl.CostEstimate(
            flops=2 * r * c * 1280, bytes_accessed=4 * r * FEAT, transcendentals=r * c
        ),
        compiler_params=pltpu.CompilerParams(vmem_limit_bytes=10 * 1024 * 1024),
        name="chunk",
    )(*operands)


def message_kernel(hidden_ref, proj_ref, alpha_ref, probes_ref, out_ref, row_ref):
    feats = jnp.dot(hidden_ref[...], proj_ref[...], preferred_element_type=jnp.float32).astype(
        jnp.bfloat16
    )
    feat_f = feats.astype(jnp.float32)
    for k in range(4):
        out_ref[k * 128 : (k + 1) * 128, :] = feats[:, k * 128 : (k + 1) * 128]
    sq = jnp.sum(feat_f * feat_f, axis=1, keepdims=True)
    hi = sq.astype(jnp.bfloat16).astype(jnp.float32)
    mid = (sq - hi).astype(jnp.bfloat16).astype(jnp.float32)
    low = sq - hi - mid
    wide = jnp.concatenate([hi, mid, low, jnp.zeros((PTS, 125), jnp.float32)], axis=1).T
    fac = jnp.concatenate(
        [alpha_ref[...].astype(jnp.float32), probes_ref[...].astype(jnp.float32), wide[0:15]],
        axis=0,
    )
    out_ref[FEAT:MSG, :] = fac.astype(jnp.bfloat16)
    for k in range(6):
        row_ref[k * 128 : (k + 1) * 128, :] = hidden_ref[:, k * 128 : (k + 1) * 128]
    row_ref[HID:ROW_MSG, :] = fac.astype(jnp.bfloat16)


def message(hidden, projection, alpha, probe_pairs):
    return pl.pallas_call(
        message_kernel,
        out_shape=(
            jax.ShapeDtypeStruct((MSG, 128), jnp.bfloat16),
            jax.ShapeDtypeStruct((ROW_MSG, 128), jnp.bfloat16),
        ),
        in_specs=[VMEM] * 4,
        out_specs=(VMEM, VMEM),
        name="message",
    )(hidden, projection, alpha.reshape(1, PTS), probe_pairs.T)


def merge_kernel(near_ref, far_ref, *out_refs):
    for k, ref in enumerate(out_refs):
        for y in range(2):
            here = slice((2 * k + y) * PTS, (2 * k + y + 1) * PTS)
            both = near_ref[here, :].astype(jnp.float32) + far_ref[here, :].astype(jnp.float32)
            ref[y] = both.astype(jnp.bfloat16)


def merge(near, far):
    n = near.shape[0] // (2 * PTS)
    return pl.pallas_call(
        merge_kernel,
        out_shape=(jax.ShapeDtypeStruct((2, PTS, FEAT), jnp.bfloat16),) * n,
        in_specs=[VMEM, VMEM],
        out_specs=(VMEM,) * n,
        compiler_params=pltpu.CompilerParams(vmem_limit_bytes=10 * 1024 * 1024),
        name="merge",
    )(near, far)


def halve_kernel(partial_ref, mine_ref, other_ref):
    first = lax.axis_index("c") == 0
    for k in range(mine_ref.shape[0]):
        a, b = partial_ref[k * 48 : k * 48 + 24, :], partial_ref[k * 48 + 24 : k * 48 + 48, :]
        mine_ref[k] = jnp.where(first, a, b)
        other_ref[k] = jnp.where(first, b, a)


def halve(partial):
    half = jax.ShapeDtypeStruct((16, 24, FEAT), jnp.bfloat16)
    return pl.pallas_call(
        halve_kernel,
        out_shape=(half, half),
        in_specs=[VMEM],
        out_specs=(VMEM, VMEM),
        compiler_params=pltpu.CompilerParams(vmem_limit_bytes=10 * 1024 * 1024),
        name="halve",
    )(partial)


def spread_kernel(got_ref, out_ref):
    total = got_ref[0].astype(jnp.float32)
    for z in range(1, got_ref.shape[0]):
        total = total + got_ref[z].astype(jnp.float32)
    for k in range(out_ref.shape[0]):
        out_ref[k] = total.astype(jnp.bfloat16)


def spread(got):
    return pl.pallas_call(
        spread_kernel,
        out_shape=jax.ShapeDtypeStruct((8, 24, FEAT), jnp.bfloat16),
        in_specs=[VMEM],
        out_specs=VMEM,
        compiler_params=pltpu.CompilerParams(vmem_limit_bytes=10 * 1024 * 1024),
        name="spread",
    )(got)


def shifted(x, axis, by):
    n = lax.axis_size(axis)
    return lax.ppermute(x, axis, [(i, (i + by) % n) for i in range(n)])


def apart(x):
    n = lax.axis_size("z")
    hops = [(2 * i + c, 2 * ((i + (1, -1)[c]) % n) + c) for i in range(n) for c in range(2)]
    return lax.ppermute(x, ("z", "c"), hops)


def steps(hidden, projection, alpha, probe_pairs, amplitude, length_sq):
    msg, row_msg = message(hidden, projection, alpha, probe_pairs)
    pair_rows = jnp.concatenate([row_msg, shifted(row_msg, "yl", 1)], axis=0)
    near = [pair_rows] + [shifted(pair_rows, "x", k) for k in (1, 2, 3)]
    far = [shifted(b, "c", 1) for b in near]
    hidden_near, *prepared = prepare(near, projection, length_sq)
    hidden_far, *more = prepare(far, projection, length_sq)
    prepared += more
    ring = [jnp.concatenate([msg, shifted(msg, "c", 1)], axis=0)]
    for k in range(1, 5):
        ring.append(apart(ring[-1] if k < 4 else ring[-1][:MSG]))
    crossed = [shifted(b, "yh", 1) for b in [msg] + ring[1:]]
    groups = [[msg, ring[1], crossed[0]], ring[2:4], crossed[1:3], [ring[4]] + crossed[3:5]]
    sums = None
    for k, group in enumerate(groups):
        sums = chunk(sums, prepared, group, amplitude, length_sq, k == 3)
    near_diff, far_diff = sums
    across_rows = (((0,), (0,)), ((), ()))
    partial = lax.dot_general(
        hidden_near, near_diff, across_rows, preferred_element_type=jnp.float32
    )
    partial += lax.dot_general(
        hidden_far, far_diff, across_rows, preferred_element_type=jnp.float32
    )
    partial = partial.astype(jnp.bfloat16)
    parts = merge(near_diff, shifted(far_diff, "c", 1))
    owned = [shifted(parts[k], "x", -k) for k in (1, 2, 3)]
    total = parts[0].astype(jnp.float32)
    for piece in owned:
        total = total + piece.astype(jnp.float32)
    aside = shifted(total[1].astype(jnp.bfloat16), "yl", 1)
    grad_feat = (total[0] + aside.astype(jnp.float32)).astype(jnp.bfloat16)
    grad_hidden = jnp.dot(grad_feat, projection.T, preferred_element_type=jnp.float32).astype(
        jnp.bfloat16
    )
    mine, other = halve(partial)
    core_sum = mine + shifted(other, "c", 1)
    got = lax.all_to_all(core_sum, ("yh", "z"), 0, 0, tiled=True)
    got = lax.all_to_all(spread(got), ("x", "yl"), 0, 0, tiled=True)
    grad_proj = got.astype(jnp.float32).sum(axis=0)
    return grad_hidden, grad_proj


def solution(mesh):
    fine = Mesh(mesh.devices.reshape(2, 8, 2, 4, 2), ALL)
    placed = (P(ALL, None), P(), P(ALL), P(ALL, None), P(), P())
    return jax.shard_map(
        steps,
        mesh=fine,
        in_specs=placed,
        out_specs=(P(ALL, None), P(("yh", "z", "c"), None)),
        check_vma=False,
    )
```
